8 devices in a mesh: frag: 2 (over z, y), dev: 4 (over x, core).
Axes of the slice: x: 2, y: 2, z: 1, core: 2. Of those that a mesh axis runs over, the one named last changes fastest.
Arguments:
- a_ints: bfloat16 [192, 96, 96, 96], P(('frag', 'dev')), parts along dimension 0
- c_occ: bfloat16 [192, 20], P('frag'), parts along dimension 0
- c_vir: bfloat16 [192, 75], P('frag'), parts along dimension 0
- eps_occ: float32 [40], P('frag'), parts along dimension 0
- eps_vir: float32 [150], P('frag'), parts along dimension 0
Outputs:
- output: float32 [40, 20], P('frag', 'dev'), parts along dimension 0
There are 2 independent parts. The reference program is written for one: setup_inputs(seed, part) draws one part's arguments, and reference() takes and returns one part's arrays. A program takes and returns all parts, laid end to end along the dimension named above; each array names one.
All inputs are finite; a program needn't handle non-finite values.
Results may differ from the reference program's by a relative error of at most 0.001.
Values are sent between devices in bfloat16 or wider.
A program may use at most 1 GiB of HBM per device.

```python
import jax
import jax.numpy as jnp
from jax import lax

PAD_BASIS = 96
NUM_OCC = 20
NUM_VIRT = 75


def setup_inputs(seed: int = 0, part: int = 0) -> dict:
    key_base = jax.random.fold_in(jax.random.key(seed), part)
    key_ints, key_occ, key_vir, key_eocc, key_evir = jax.random.split(key_base, 5)

    def draw_row(row_idx):
        raw_row = jax.random.normal(jax.random.fold_in(key_ints, row_idx), (PAD_BASIS, PAD_BASIS, PAD_BASIS), jnp.float32)
        mixed_row = (raw_row + 0.5 * jnp.transpose(raw_row, (2, 1, 0))) * (1.25 ** -0.5)
        return mixed_row.astype(jnp.bfloat16)

    a_ints = lax.map(draw_row, jnp.arange(PAD_BASIS))
    c_occ = (jax.random.normal(key_occ, (PAD_BASIS, NUM_OCC), jnp.float32) * PAD_BASIS ** -0.5).astype(jnp.bfloat16)
    c_vir = (jax.random.normal(key_vir, (PAD_BASIS, NUM_VIRT), jnp.float32) * (PAD_BASIS * NUM_VIRT) ** -0.5).astype(jnp.bfloat16)
    eps_occ = jax.random.uniform(key_eocc, (NUM_OCC,), jnp.float32, -1.5, -0.5)
    eps_vir = jax.random.uniform(key_evir, (NUM_VIRT,), jnp.float32, 0.3, 2.0)
    return {"a_ints": a_ints, "c_occ": c_occ, "c_vir": c_vir, "eps_occ": eps_occ, "eps_vir": eps_vir}


def reference(a_ints, c_occ, c_vir, eps_occ, eps_vir):
    occ_32 = c_occ.astype(jnp.float32)
    vir_32 = c_vir.astype(jnp.float32)

    def first_half(a_row):
        t_one = jnp.einsum("qrs,rj->qsj", a_row.astype(jnp.float32), occ_32).astype(jnp.bfloat16)
        return jnp.einsum("qsj,sb->qjb", t_one.astype(jnp.float32), vir_32).astype(jnp.bfloat16)

    half_mo = lax.map(first_half, a_ints)
    g_mat = jnp.einsum("pqjb,qa->pjba", half_mo.astype(jnp.float32), vir_32).astype(jnp.bfloat16)
    v_mo = jnp.einsum("pjba,pi->jbai", g_mat.astype(jnp.float32), occ_32)
    v_swap = jnp.swapaxes(v_mo, 1, 2)
    denominator = (eps_occ[:, None, None, None] + eps_occ[None, None, None, :]
                   - eps_vir[None, :, None, None] - eps_vir[None, None, :, None])
    pair_ji = jnp.sum(v_mo * (2.0 * v_mo - v_swap) / denominator, axis=(1, 2))
    return pair_ji.T
```

```python
import functools

import jax
import jax.numpy as jnp
from jax import lax
from jax.experimental import pallas as pl
from jax.experimental.pallas import tpu as pltpu
from jax.sharding import PartitionSpec as P

MESH = pl.DeviceIdType.MESH
F32, BF16 = jnp.float32, jnp.bfloat16

N = 96
O = 20
V = 75
NDEV = 4
NP = N // NDEV
OD = O // NDEV
L = 128
JB = 384
PC = 4
NC = NP // PC
AQ = 19
GR = AQ * 4 * PC
SLOTS = 3


def _dot(x, y):
    return jnp.dot(x, y, preferred_element_type=F32)


def _div(x, d):
    return jnp.floor((x + 0.5) * (1.0 / d))


def _rows(shape):
    return lax.broadcasted_iota(jnp.int32, shape, 0).astype(F32)


def _cols(shape):
    return lax.broadcasted_iota(jnp.int32, shape, 1).astype(F32)


def _onehot(cond):
    return jnp.where(cond, 1.0, 0.0).astype(BF16)


def _spread(m, row_of, col_of, keep, shape):
    r_shape, c_shape = (shape[0], m.shape[0]), (m.shape[1], shape[1])
    left = _onehot(row_of(_rows(r_shape)) == _cols(r_shape))
    right = _onehot(_rows(c_shape) == col_of(_cols(c_shape)))
    full = _dot(_dot(left, m).astype(BF16), right)
    return jnp.where(keep(_rows(shape), _cols(shape)), full, 0.0).astype(BF16)


def kernel(a_hbm, co_ref, cv_ref, eo_ref, ev_ref, out_ref, a_buf, l1, w2, l3, l4, t_s, h_s, g_send, g_recv,
           v_s, r_s, e_s, a_sem, send_sem, recv_sem):
    f, me = lax.axis_index("frag"), lax.axis_index("dev")
    chip, core = me // 2, lax.rem(me, 2)
    far0 = (1 - chip) * 2 + core
    far1 = (1 - chip) * 2 + 1 - core
    near = chip * 2 + 1 - core
    peers = (far0, far1, near)

    def a_copy(p, slot):
        return pltpu.make_async_copy(a_hbm.at[p], a_buf.at[slot], a_sem.at[slot])

    for s in range(SLOTS):
        a_copy(s, s).start()

    barrier = pltpu.get_barrier_semaphore()
    for d in peers:
        pl.semaphore_signal(barrier, inc=1, device_id=(f, d), device_id_type=MESH)

    co, cv = co_ref[...], cv_ref[...]
    mod = lambda x, d: x - d * _div(x, d)
    l1[...] = _spread(co, lambda x: mod(x, O), lambda y: mod(y, N), lambda x, y: _div(x, O) == _div(y, N), (2 * O, 2 * N))
    cv_t = cv.astype(F32).T.astype(BF16)
    for jj in range(OD):
        w2[jj * L:(jj + 1) * L, :] = _spread(
            cv_t, lambda x: x, lambda y: y - V * jj, lambda x, y: x < N, (L, JB))
    l3[...] = _spread(cv, lambda x: _div(x, PC), lambda y: mod(y, N), lambda x, y: mod(x, PC) == _div(y, N), (GR, PC * N))
    l4[...] = _spread(co, lambda x: mod(x, O), lambda y: _div(y, 16) * PC + mod(y, PC),
                      lambda x, y: _div(x, O) == _div(mod(y, 16), PC), (4 * O, N * 4))

    pl.semaphore_wait(barrier, 3)

    def send(c, k):
        return pltpu.make_async_remote_copy(
            src_ref=g_send.at[c, k], dst_ref=g_recv.at[me, c], send_sem=send_sem.at[c, k],
            recv_sem=recv_sem.at[me, c], device_id=(f, peers[k]), device_id_type=MESH)

    def step_p(p, _):
        slot = lax.rem(p, SLOTS)
        a_copy(p, slot).wait()
        lhs = l1[...]
        for q in range(0, N, 4):
            x0 = jnp.pad(a_buf[slot, q:q + 2].reshape(2 * N, N), ((0, 0), (0, L - N)))
            x1 = jnp.pad(a_buf[slot, q + 2:q + 4].reshape(2 * N, N), ((0, 0), (0, L - N)))
            t = _dot(lhs, jnp.concatenate([x0, x1], axis=1))
            t_s[q * O:(q + 2) * O, :] = t[:, :L]
            t_s[(q + 2) * O:(q + 4) * O, :] = t[:, L:]

        @pl.when(p + SLOTS < NP)
        def _():
            a_copy(p + SLOTS, slot).start()

        pc = lax.rem(p, PC)
        rows = pl.ds(pl.multiple_of(pc * N, N), N)
        for d in range(NDEV):
            x = [t_s[pl.ds(d * OD + jj, N, stride=O), :].astype(BF16) for jj in range(OD)]
            h_s[d, rows, :256] = _dot(jnp.concatenate(x[:4], axis=1), w2[:4 * L, :256]).astype(BF16)
            h_s[d, rows, 256:] = _dot(jnp.concatenate(x[2:], axis=1), w2[2 * L:, 256:]).astype(BF16)

        @pl.when(pc == PC - 1)
        def _():
            c = p // PC
            for k in range(3):
                g_send[c, k] = _dot(l3[...], h_s[peers[k]]).astype(BF16)
                send(c, k).start()
            g_recv[me, c] = _dot(l3[...], h_s[me]).astype(BF16)
        return 0

    lax.fori_loop(0, NP, step_p, 0)

    ev = jnp.broadcast_to(ev_ref[...], (L, V))
    ev = jnp.pad(ev, ((0, 0), (0, L - V)))
    pair = ev + ev.T
    inside = (_rows((80, L)) < V) & (_cols((80, L)) < V)

    def recip(i, _):
        for jj in range(OD):
            den = (eo_ref[i] + eo_ref[me * OD + jj]) - pair[:80]
            r_s[i * OD + jj] = jnp.where(inside, 1.0 / den, 0.0)
        return 0

    lax.fori_loop(0, O, recip, 0)
    v_s[:, 4 * AQ * O:, :] = jnp.zeros((3, 4 * O, L), F32)

    for c in range(NC):
        for k in range(3):
            d = peers[k]
            pltpu.make_async_remote_copy(
                src_ref=g_send.at[c, k], dst_ref=g_recv.at[d, c], send_sem=send_sem.at[c, k],
                recv_sem=recv_sem.at[d, c], device_id=(f, d), device_id_type=MESH).wait()

    def contract(t, _):
        rows = pl.ds(pl.multiple_of(t * 16, 16), 16)
        g = g_recv[:, :, rows, :].reshape(NDEV * NC * 16, JB)
        v = _dot(l4[...], g)
        for n in range(3):
            v_s[n, pl.ds(pl.multiple_of(t * 4 * O, 4 * O), 4 * O), :] = v[:, n * L:(n + 1) * L]
        return 0

    lax.fori_loop(0, AQ, contract, 0)

    def energy(i, _):
        tiles = [v_s[t, pl.ds(i, 80, stride=O), :] for t in range(3)]
        lane = lax.broadcasted_iota(jnp.int32, (80, L), 1)
        for jj in range(OD):
            t, off = divmod(V * jj, L)
            m = pltpu.roll(tiles[t], (L - off) % L, axis=1) if off else tiles[t]
            if off + V > L:
                m = jnp.where(lane < L - off, m, pltpu.roll(tiles[t + 1], L - off, axis=1))
            mt = jnp.pad(m, ((0, L - 80), (0, 0))).T[:80]
            term = m * (2.0 * m - mt) * r_s[i * OD + jj]
            e_s[jj, pl.ds(pl.multiple_of(i * 8, 8), 8), :] = jnp.sum(term.reshape(10, 8, L), axis=0)
        return 0

    lax.fori_loop(0, O, energy, 0)
    for jj in range(OD):
        tot = e_s[jj, pl.ds(0, O, stride=8), :]
        for s in range(1, 8):
            tot = tot + e_s[jj, pl.ds(s, O, stride=8), :]
        col = jnp.sum(jnp.pad(tot, ((0, 32 - O), (0, 0))).T, axis=0, keepdims=True)
        out_ref[jj:jj + 1, :] = col[:, :O]


def solution(mesh):
    def per_device(a_ints, c_occ, c_vir, eps_occ, eps_vir):
        vm = pl.BlockSpec(memory_space=pltpu.VMEM)
        e = pl.pallas_call(
            kernel,
            out_shape=jax.ShapeDtypeStruct((OD, O), F32),
            in_specs=[pl.BlockSpec(memory_space=pl.ANY), vm, vm, pl.BlockSpec(memory_space=pltpu.SMEM), vm],
            out_specs=vm,
            scratch_shapes=[
                pltpu.VMEM((SLOTS, N, N, N), BF16),
                pltpu.VMEM((2 * O, 2 * N), BF16),
                pltpu.VMEM((OD * L, JB), BF16),
                pltpu.VMEM((GR, PC * N), BF16),
                pltpu.VMEM((4 * O, 4 * N), BF16),
                pltpu.VMEM((N * O, L), F32),
                pltpu.VMEM((NDEV, PC * N, JB), BF16),
                pltpu.VMEM((NC, 3, GR, JB), BF16),
                pltpu.VMEM((NDEV, NC, GR, JB), BF16),
                pltpu.VMEM((3, 80 * O, L), F32),
                pltpu.VMEM((O * OD, 80, L), F32),
                pltpu.VMEM((OD, O * 8, L), F32),
                pltpu.SemaphoreType.DMA((SLOTS,)),
                pltpu.SemaphoreType.DMA((NC, 3)),
                pltpu.SemaphoreType.DMA((NDEV, NC)),
            ],
            compiler_params=pltpu.CompilerParams(
                collective_id=0, has_side_effects=True, vmem_limit_bytes=60 * 2**20),
        )(a_ints, c_occ.T, c_vir.T, eps_occ, eps_vir.reshape(1, V))
        return e.T

    return jax.shard_map(
        per_device,
        mesh=mesh,
        in_specs=(P(("frag", "dev")), P("frag"), P("frag"), P("frag"), P("frag")),
        out_specs=P("frag", "dev"),
        check_vma=False,
    )
```

```python
import functools

import jax
import jax.numpy as jnp
from jax import lax
from jax.experimental import pallas as pl
from jax.experimental.pallas import tpu as pltpu
from jax.sharding import PartitionSpec as P

MESH = pl.DeviceIdType.MESH
F32, BF16 = jnp.float32, jnp.bfloat16

N = 96
O = 20
V = 75
NDEV = 4
NP = N // NDEV
OD = O // NDEV
L = 128
JB = 384
PC = 4
NC = NP // PC
AQ = 19
GR = AQ * 4 * PC
SLOTS = 6
T1 = 10
GH = T1 * 16
XR = GR - GH
VQ = AQ - T1
IG = O // 2


def _dot(x, y):
    return jnp.dot(x, y, preferred_element_type=F32)


def _div(x, d):
    return jnp.floor((x + 0.5) * (1.0 / d))


def _rows(shape):
    return lax.broadcasted_iota(jnp.int32, shape, 0).astype(F32)


def _cols(shape):
    return lax.broadcasted_iota(jnp.int32, shape, 1).astype(F32)


def _onehot(cond):
    return jnp.where(cond, 1.0, 0.0).astype(BF16)


def _spread(m, row_of, col_of, keep, shape):
    r_shape, c_shape = (shape[0], m.shape[0]), (m.shape[1], shape[1])
    left = _onehot(row_of(_rows(r_shape)) == _cols(r_shape))
    right = _onehot(_rows(c_shape) == col_of(_cols(c_shape)))
    full = _dot(_dot(left, m).astype(BF16), right)
    return jnp.where(keep(_rows(shape), _cols(shape)), full, 0.0).astype(BF16)


def kernel(a_hbm, co_ref, cv_ref, eo_ref, ev_ref, out_ref, a_buf, l1, w2, l3, l4, t_s, h_s, g_send, g_own, g_near, g_far,
           x_near, v_send, v_recv, v_s, r_s, e_s, a_sem, send_sem, far_sem, near_sem, x_sem, vs_sem, vr_sem):
    f, me = lax.axis_index("frag"), lax.axis_index("dev")
    chip, core = me // 2, lax.rem(me, 2)
    far0 = (1 - chip) * 2 + core
    far1 = (1 - chip) * 2 + 1 - core
    near = chip * 2 + 1 - core
    peers = (far0, far1, near)

    def a_copy(p, slot):
        return pltpu.make_async_copy(a_hbm.at[p], a_buf.at[slot], a_sem.at[slot])

    for s in range(SLOTS):
        a_copy(s, s).start()

    barrier = pltpu.get_barrier_semaphore()
    for d in peers:
        pl.semaphore_signal(barrier, inc=1, device_id=(f, d), device_id_type=MESH)

    co, cv = co_ref[...], cv_ref[...]
    mod = lambda x, d: x - d * _div(x, d)
    l1[...] = _spread(co, lambda x: mod(x, O), lambda y: mod(y, N), lambda x, y: _div(x, O) == _div(y, N), (2 * O, 2 * N))
    cv_t = cv.astype(F32).T.astype(BF16)
    for jj in range(OD):
        w2[jj * L:(jj + 1) * L, :] = _spread(
            cv_t, lambda x: x, lambda y: y - V * jj, lambda x, y: x < N, (L, JB))
    l3[...] = _spread(cv, lambda x: _div(x, PC), lambda y: mod(y, N), lambda x, y: mod(x, PC) == _div(y, N), (GR, PC * N))

    def source_p(y):
        slot = _div(y, N)
        src = jnp.where(slot == 0, me, jnp.where(slot == 1, near, jnp.where(slot == 2, far0, far1))).astype(F32)
        return src * NP + _div(mod(y, N), 16) * PC + mod(y, PC)

    l4[...] = _spread(co, lambda x: _div(x, 8) * 2 + mod(x, 2), source_p,
                      lambda x, y: _div(mod(x, 8), 2) == _div(mod(y, 16), PC), (4 * O, N * 4))

    def g_copy(c, k):
        return pltpu.make_async_remote_copy(
            src_ref=g_send.at[c, k, pl.ds(0, GH)], dst_ref=g_far.at[k, c], send_sem=send_sem.at[c, k],
            recv_sem=far_sem.at[k, c], device_id=(f, peers[k]), device_id_type=MESH)

    def x_copy(c):
        return pltpu.make_async_remote_copy(
            src_ref=g_send.at[c, 1, pl.ds(GH, XR)], dst_ref=x_near.at[c], send_sem=send_sem.at[c, 2],
            recv_sem=x_sem.at[c], device_id=(f, near), device_id_type=MESH)

    def n_copy(c):
        return pltpu.make_async_remote_copy(
            src_ref=g_send.at[c, 2], dst_ref=g_near.at[c], send_sem=send_sem.at[c, 3],
            recv_sem=near_sem.at[c], device_id=(f, near), device_id_type=MESH)

    def v_copy(g):
        return pltpu.make_async_remote_copy(
            src_ref=v_send.at[g], dst_ref=v_recv.at[g], send_sem=vs_sem.at[g],
            recv_sem=vr_sem.at[g], device_id=(f, far0), device_id_type=MESH)

    def step_p(p, _):
        slot = lax.rem(p, SLOTS)
        a_copy(p, slot).wait()
        lhs = l1[...]
        for q in range(0, N, 4):
            x0 = jnp.pad(a_buf[slot, q:q + 2].reshape(2 * N, N), ((0, 0), (0, L - N)))
            x1 = jnp.pad(a_buf[slot, q + 2:q + 4].reshape(2 * N, N), ((0, 0), (0, L - N)))
            t = _dot(lhs, jnp.concatenate([x0, x1], axis=1))
            t_s[q * O:(q + 2) * O, :] = t[:, :L]
            t_s[(q + 2) * O:(q + 4) * O, :] = t[:, L:]

        @pl.when(p + SLOTS < NP)
        def _():
            a_copy(p + SLOTS, slot).start()

        pc = lax.rem(p, PC)
        rows = pl.ds(pl.multiple_of(pc * N, N), N)
        for d in range(NDEV):
            x = [t_s[pl.ds(d * OD + jj, N, stride=O), :].astype(BF16) for jj in range(OD)]
            h_s[d, rows, :256] = _dot(jnp.concatenate(x[:4], axis=1), w2[:4 * L, :256]).astype(BF16)
            h_s[d, rows, 256:] = _dot(jnp.concatenate(x[2:], axis=1), w2[2 * L:, 256:]).astype(BF16)

        @pl.when(p == PC - 1)
        def _():
            pl.semaphore_wait(barrier, 3)

        @pl.when(pc == PC - 1)
        def _():
            c = p // PC
            g_send[c, 0] = _dot(l3[...], h_s[far0]).astype(BF16)
            g_copy(c, 0).start()
            g_send[c, 1] = _dot(l3[...], h_s[far1]).astype(BF16)
            g_copy(c, 1).start()
            x_copy(c).start()
            g_send[c, 2] = _dot(l3[...], h_s[near]).astype(BF16)
            n_copy(c).start()
            g_own[c] = _dot(l3[...], h_s[me]).astype(BF16)
        return 0

    lax.fori_loop(0, NP, step_p, 0)

    def quad(own, other, t):
        rows = pl.ds(pl.multiple_of(t * 16, 16), 16)
        orows = pl.ds(pl.multiple_of((t - (AQ - other.shape[1] // 16)) * 16, 16), 16)
        return jnp.concatenate([own[:, rows].reshape(N, JB), other[:, orows].reshape(N, JB)], axis=0)

    for c in range(NC):
        x_copy(c).wait_recv()

    def partial(t, _):
        v = _dot(l4[:, :2 * N], quad(g_send.at[:, 0], x_near, t))
        rows = pl.ds(pl.multiple_of((t - T1) * 8, 8), 8)
        for g in range(IG):
            for n in range(3):
                v_send[g, n, rows, :] = v[g * 8:(g + 1) * 8, n * L:(n + 1) * L]
        return 0

    lax.fori_loop(T1, AQ, partial, 0)
    for g in range(IG):
        v_copy(g).start()

    ev = jnp.broadcast_to(ev_ref[...], (L, V))
    ev = jnp.pad(ev, ((0, 0), (0, L - V)))
    pair = ev + ev.T
    inside = (_rows((80, L)) < V) & (_cols((80, L)) < V)

    def recip(i, _):
        for jj in range(OD):
            den = (eo_ref[i] + eo_ref[me * OD + jj]) - pair[:80]
            r_s[i * OD + jj] = jnp.where(inside, 1.0 / den, 0.0)
        return 0

    lax.fori_loop(0, O, recip, 0)

    v_s[:, :, AQ * 8:, :] = jnp.zeros((IG, 3, 8, L), F32)
    for c in range(NC):
        n_copy(c).wait_recv()

    def contract(t, _):
        v = _dot(l4[:, :2 * N], quad(g_own, g_near, t))
        rows = pl.ds(pl.multiple_of(t * 8, 8), 8)
        for g in range(IG):
            for n in range(3):
                v_s[g, n, rows, :] = v[g * 8:(g + 1) * 8, n * L:(n + 1) * L]
        return 0

    lax.fori_loop(0, AQ, contract, 0)
    for c in range(NC):
        for k in range(2):
            g_copy(c, k).wait_recv()

    def contract_far(t, _):
        rows = pl.ds(pl.multiple_of(t * 16, 16), 16)
        v = _dot(l4[:, 2 * N:], g_far[:, :, rows].reshape(2 * N, JB))
        rows = pl.ds(pl.multiple_of(t * 8, 8), 8)
        for g in range(IG):
            for n in range(3):
                v_s[g, n, rows, :] += v[g * 8:(g + 1) * 8, n * L:(n + 1) * L]
        return 0

    lax.fori_loop(0, T1, contract_far, 0)

    def energy(g, _):
        v_copy(g).wait_recv()
        v_s[g, :, T1 * 8:AQ * 8, :] += v_recv[g]
        lane = lax.broadcasted_iota(jnp.int32, (80, L), 1)
        for ii in range(2):
            i = g * 2 + ii
            tiles = [v_s[g, n, pl.ds(ii, 80, stride=2), :] for n in range(3)]
            for jj in range(OD):
                t, off = divmod(V * jj, L)
                m = pltpu.roll(tiles[t], (L - off) % L, axis=1) if off else tiles[t]
                if off + V > L:
                    m = jnp.where(lane < L - off, m, pltpu.roll(tiles[t + 1], L - off, axis=1))
                mt = jnp.pad(m, ((0, L - 80), (0, 0))).T[:80]
                term = m * (2.0 * m - mt) * r_s[i * OD + jj]
                e_s[jj, pl.ds(pl.multiple_of(i * 8, 8), 8), :] = jnp.sum(term.reshape(10, 8, L), axis=0)
        return 0

    lax.fori_loop(0, IG, energy, 0)
    for jj in range(OD):
        tot = e_s[jj, pl.ds(0, O, stride=8), :]
        for s in range(1, 8):
            tot = tot + e_s[jj, pl.ds(s, O, stride=8), :]
        col = jnp.sum(jnp.pad(tot, ((0, 32 - O), (0, 0))).T, axis=0, keepdims=True)
        out_ref[jj:jj + 1, :] = col[:, :O]

    for c in range(NC):
        g_copy(c, 0).wait_send()
        g_copy(c, 1).wait_send()
        x_copy(c).wait_send()
        n_copy(c).wait_send()
    for g in range(IG):
        v_copy(g).wait_send()


def solution(mesh):
    def per_device(a_ints, c_occ, c_vir, eps_occ, eps_vir):
        vm = pl.BlockSpec(memory_space=pltpu.VMEM)
        e = pl.pallas_call(
            kernel,
            out_shape=jax.ShapeDtypeStruct((OD, O), F32),
            in_specs=[pl.BlockSpec(memory_space=pl.ANY), vm, vm, pl.BlockSpec(memory_space=pltpu.SMEM), vm],
            out_specs=vm,
            scratch_shapes=[
                pltpu.VMEM((SLOTS, N, N, N), BF16),
                pltpu.VMEM((2 * O, 2 * N), BF16),
                pltpu.VMEM((OD * L, JB), BF16),
                pltpu.VMEM((GR, PC * N), BF16),
                pltpu.VMEM((4 * O, 4 * N), BF16),
                pltpu.VMEM((N * O, L), F32),
                pltpu.VMEM((NDEV, PC * N, JB), BF16),
                pltpu.VMEM((NC, 3, GR, JB), BF16),
                pltpu.VMEM((NC, GR, JB), BF16),
                pltpu.VMEM((NC, GR, JB), BF16),
                pltpu.VMEM((2, NC, GH, JB), BF16),
                pltpu.VMEM((NC, XR, JB), BF16),
                pltpu.VMEM((IG, 3, VQ * 8, L), F32),
                pltpu.VMEM((IG, 3, VQ * 8, L), F32),
                pltpu.VMEM((IG, 3, 160, L), F32),
                pltpu.VMEM((O * OD, 80, L), F32),
                pltpu.VMEM((OD, O * 8, L), F32),
                pltpu.SemaphoreType.DMA((SLOTS,)),
                pltpu.SemaphoreType.DMA((NC, 4)),
                pltpu.SemaphoreType.DMA((2, NC)),
                pltpu.SemaphoreType.DMA((NC,)),
                pltpu.SemaphoreType.DMA((NC,)),
                pltpu.SemaphoreType.DMA((IG,)),
                pltpu.SemaphoreType.DMA((IG,)),
            ],
            compiler_params=pltpu.CompilerParams(
                collective_id=0, has_side_effects=True, vmem_limit_bytes=60 * 2**20),
        )(a_ints, c_occ.T, c_vir.T, eps_occ, eps_vir.reshape(1, V))
        return e.T

    return jax.shard_map(
        per_device,
        mesh=mesh,
        in_specs=(P(("frag", "dev")), P("frag"), P("frag"), P("frag"), P("frag")),
        out_specs=P("frag", "dev"),
        check_vma=False,
    )
```

```python
import functools

import jax
import jax.numpy as jnp
from jax import lax
from jax.experimental import pallas as pl
from jax.experimental.pallas import tpu as pltpu
from jax.sharding import PartitionSpec as P

MESH = pl.DeviceIdType.MESH
F32, BF16 = jnp.float32, jnp.bfloat16

N = 96
O = 20
V = 75
NDEV = 4
NP = N // NDEV
OD = O // NDEV
L = 128
JB = 384
PC = 2
NC = NP // PC
AO = 10
GR = AO * 8 * PC
AV = 76
SLOTS = 6
U1 = 4
GH = U1 * 16
XR = GR - GH
VR = (AV - U1 * 8) * 2
IG = O // 2


def _dot(x, y):
    return jnp.dot(x, y, preferred_element_type=F32)


def _div(x, d):
    return jnp.floor((x + 0.5) * (1.0 / d))


def _rows(shape):
    return lax.broadcasted_iota(jnp.int32, shape, 0).astype(F32)


def _cols(shape):
    return lax.broadcasted_iota(jnp.int32, shape, 1).astype(F32)


def _onehot(cond):
    return jnp.where(cond, 1.0, 0.0).astype(BF16)


def _spread(m, row_of, col_of, keep, shape):
    r_shape, c_shape = (shape[0], m.shape[0]), (m.shape[1], shape[1])
    left = _onehot(row_of(_rows(r_shape)) == _cols(r_shape))
    right = _onehot(_rows(c_shape) == col_of(_cols(c_shape)))
    full = _dot(_dot(left, m).astype(BF16), right)
    return jnp.where(keep(_rows(shape), _cols(shape)), full, 0.0).astype(BF16)


def kernel(a_hbm, co_hbm, cv_hbm, eo_hbm, ev_hbm, out_ref, co_ref, cv_ref, eo_ref, ev_ref, a_buf, l1, w2, l3, l4, l4f,
           t0_s, t1_s, h_s, g_send, g_own, g_near, g_far, x_near, v_send, v_recv, v_s, r_s, e_s,
           a_sem, in_sem, send_sem, far_sem, near_sem, x_sem, vs_sem, vr_sem):
    f, me = lax.axis_index("frag"), lax.axis_index("dev")
    chip, core = me // 2, lax.rem(me, 2)
    far0 = (1 - chip) * 2 + core
    far1 = (1 - chip) * 2 + 1 - core
    near = chip * 2 + 1 - core
    peers = (far0, far1, near)

    def a_copy(p, slot):
        return pltpu.make_async_copy(a_hbm.at[p], a_buf.at[slot], a_sem.at[slot])

    barrier = pltpu.get_barrier_semaphore()
    for d in peers:
        pl.semaphore_signal(barrier, inc=1, device_id=(f, d), device_id_type=MESH)
    small = [pltpu.make_async_copy(x, y, in_sem.at[k]) for k, (x, y) in enumerate(
        [(co_hbm, co_ref), (cv_hbm, cv_ref), (eo_hbm, eo_ref), (ev_hbm, ev_ref)])]
    for cp in small[:2]:
        cp.start()
    a_copy(0, 0).start()
    for cp in small[:2]:
        cp.wait()
    for s in range(1, SLOTS):
        a_copy(s, s).start()
    for cp in small[2:]:
        cp.start()

    co, cv = co_ref[...], cv_ref[...]
    mod = lambda x, d: x - d * _div(x, d)
    co_pad = jnp.pad(co.astype(F32), ((0, O), (0, 256 - N)))
    l1[...] = (co_pad + pltpu.roll(pltpu.roll(co_pad, O, axis=0), N, axis=1)).astype(BF16)[:, :2 * N]
    cv_t = jnp.pad(cv.astype(F32), ((0, L - V), (0, L - N))).T
    cv_pad = jnp.pad(cv_t, ((0, 0), (0, JB - L)))
    for jj in range(OD):
        w2[jj * L:(jj + 1) * L, :] = (pltpu.roll(cv_pad, V * jj, axis=1) if jj else cv_pad).astype(BF16)
    l3[...] = _spread(cv, lambda x: _div(x, PC), lambda y: mod(y, N), lambda x, y: mod(x, PC) == _div(y, N), (GR, PC * N))

    def spread_co(slot0, slot1):
        return _spread(
            co, lambda x: _div(x, 16) * 2 + mod(x, 2),
            lambda y: jnp.where(y < NC * 16, slot0, slot1).astype(F32) * NP + _div(mod(y, NC * 16), 16) * PC + mod(y, PC),
            lambda x, y: _div(mod(x, 16), 2) == _div(mod(y, 16), PC), (8 * O, 2 * NC * 16))

    def g_copy(c, k):
        return pltpu.make_async_remote_copy(
            src_ref=g_send.at[c, k, pl.ds(0, GH)], dst_ref=g_far.at[k, c], send_sem=send_sem.at[c, k],
            recv_sem=far_sem.at[k, c], device_id=(f, peers[k]), device_id_type=MESH)

    def x_copy(c):
        return pltpu.make_async_remote_copy(
            src_ref=g_send.at[c, 1, pl.ds(GH, XR)], dst_ref=x_near.at[c], send_sem=send_sem.at[c, 2],
            recv_sem=x_sem.at[c], device_id=(f, near), device_id_type=MESH)

    def n_copy(c):
        return pltpu.make_async_remote_copy(
            src_ref=g_send.at[c, 2], dst_ref=g_near.at[c], send_sem=send_sem.at[c, 3],
            recv_sem=near_sem.at[c], device_id=(f, near), device_id_type=MESH)

    def v_copy(g):
        return pltpu.make_async_remote_copy(
            src_ref=v_send.at[g], dst_ref=v_recv.at[g], send_sem=vs_sem.at[g],
            recv_sem=vr_sem.at[g], device_id=(f, far0), device_id_type=MESH)

    def first_step(slot, buf, q):
        x0 = jnp.pad(a_buf[slot, q:q + 2].reshape(2 * N, N), ((0, 0), (0, L - N)))
        x1 = jnp.pad(a_buf[slot, q + 2:q + 4].reshape(2 * N, N), ((0, 0), (0, L - N)))
        t = _dot(l1[...], jnp.concatenate([x0, x1], axis=1))
        buf[q * O:(q + 2) * O, :] = t[:, :L]
        buf[(q + 2) * O:(q + 4) * O, :] = t[:, L:]

    def second_step(buf, row):
        x = [jnp.concatenate([buf[pl.ds(d * OD + jj, N, stride=O), :].astype(BF16) for d in range(NDEV)], axis=0)
             for jj in range(OD)]
        h0 = _dot(jnp.concatenate(x[:4], axis=1), w2[:4 * L, :256]).astype(BF16)
        h1 = _dot(jnp.concatenate(x[2:], axis=1), w2[2 * L:, 256:]).astype(BF16)
        for d in range(NDEV):
            h_s[d, row * N:(row + 1) * N, :256] = h0[d * N:(d + 1) * N]
            h_s[d, row * N:(row + 1) * N, 256:] = h1[d * N:(d + 1) * N]

    def third_step(d):
        return _dot(l3[...], h_s[d]).astype(BF16)

    def chunk(c, _):
        p = c * PC
        slot = lax.rem(p, SLOTS)
        a_copy(p, slot).wait()
        for q in range(0, N, 4):
            first_step(slot, t0_s, q)
        a_copy(p + 1, slot + 1).wait()
        for q in range(0, N, 4):
            first_step(slot + 1, t1_s, q)
            if q == 8:
                second_step(t0_s, 0)

        second_step(t1_s, 1)
        g_send[c, 0] = third_step(far0)
        g_send[c, 1] = third_step(far1)
        g_send[c, 2] = third_step(near)
        g_own[c] = third_step(me)

        @pl.when(c == 0)
        def _():
            pl.semaphore_wait(barrier, 3)

        x_copy(c).start()
        g_copy(c, 0).start()
        g_copy(c, 1).start()
        n_copy(c).start()

        @pl.when(p + SLOTS < NP)
        def _():
            a_copy(p + SLOTS, slot).start()
            a_copy(p + 1 + SLOTS, slot + 1).start()

        return 0

    lax.fori_loop(0, NC, chunk, 0)

    l4[...] = spread_co(me, near)

    def octet(own, other, t, t_other):
        rows = pl.ds(pl.multiple_of(t * 16, 16), 16)
        orows = pl.ds(pl.multiple_of(t_other * 16, 16), 16)
        return jnp.concatenate([own[:, rows].reshape(NC * 16, JB), other[:, orows].reshape(NC * 16, JB)], axis=0)

    for c in range(NC):
        x_copy(c).wait_recv()

    def partial(t):
        v = _dot(l4[...], octet(g_send.at[:, 0], x_near, t, t - U1))
        r = min(16, AV * 2 - t * 16)
        for g in range(IG):
            for n in range(3):
                v_send[g, n, (t - U1) * 16:(t - U1) * 16 + r, :] = v[g * 16:g * 16 + r, n * L:(n + 1) * L]

    for t in range(U1, AO):
        partial(t)
    for g in range(IG):
        v_copy(g).start()

    l4f[...] = spread_co(far0, far1)

    for cp in small[2:]:
        cp.wait()
    ev = jnp.broadcast_to(ev_ref[...], (L, V))
    ev = jnp.pad(ev, ((0, 0), (0, L - V)))
    pair = ev + ev.T
    inside = (_rows((80, L)) < V) & (_cols((80, L)) < V)

    def recip(i, _):
        for jj in range(OD):
            den = (eo_ref[i] + eo_ref[me * OD + jj]) - pair[:80]
            r_s[i * OD + jj] = jnp.where(inside, 1.0 / den, 0.0)
        return 0

    lax.fori_loop(0, O, recip, 0)

    for c in range(NC):
        n_copy(c).wait_recv()

    def contract(t, _):
        v = _dot(l4[...], octet(g_own, g_near, t, t))
        rows = pl.ds(pl.multiple_of(t * 16, 16), 16)
        for g in range(IG):
            for n in range(3):
                v_s[g, n, rows, :] = v[g * 16:(g + 1) * 16, n * L:(n + 1) * L]
        return 0

    lax.fori_loop(0, AO, contract, 0)
    for c in range(NC):
        for k in range(2):
            g_copy(c, k).wait_recv()

    def contract_far(t, _):
        v = _dot(l4f[...], octet(g_far.at[0], g_far.at[1], t, t))
        rows = pl.ds(pl.multiple_of(t * 16, 16), 16)
        for g in range(IG):
            for n in range(3):
                v_s[g, n, rows, :] += v[g * 16:(g + 1) * 16, n * L:(n + 1) * L]
        return 0

    lax.fori_loop(0, U1, contract_far, 0)

    def energy(g, _):
        v_copy(g).wait_recv()
        v_s[g, :, U1 * 16:AV * 2, :] += v_recv[g]
        lane = lax.broadcasted_iota(jnp.int32, (80, L), 1)
        for ii in range(2):
            i = g * 2 + ii
            tiles = [v_s[g, n, pl.ds(ii, 80, stride=2), :] for n in range(3)]
            for jj in range(OD):
                t, off = divmod(V * jj, L)
                m = pltpu.roll(tiles[t], (L - off) % L, axis=1) if off else tiles[t]
                if off + V > L:
                    m = jnp.where(lane < L - off, m, pltpu.roll(tiles[t + 1], L - off, axis=1))
                mt = jnp.pad(m, ((0, L - 80), (0, 0))).T[:80]
                term = m * (2.0 * m - mt) * r_s[i * OD + jj]
                e_s[jj, pl.ds(pl.multiple_of(i * 8, 8), 8), :] = jnp.sum(term.reshape(10, 8, L), axis=0)
        return 0

    lax.fori_loop(0, IG, energy, 0)
    for jj in range(OD):
        tot = e_s[jj, pl.ds(0, O, stride=8), :]
        for s in range(1, 8):
            tot = tot + e_s[jj, pl.ds(s, O, stride=8), :]
        col = jnp.sum(jnp.pad(tot, ((0, 32 - O), (0, 0))).T, axis=0, keepdims=True)
        out_ref[jj:jj + 1, :] = col[:, :O]

    for c in range(NC):
        g_copy(c, 0).wait_send()
        g_copy(c, 1).wait_send()
        x_copy(c).wait_send()
        n_copy(c).wait_send()
    for g in range(IG):
        v_copy(g).wait_send()


def solution(mesh):
    def per_device(a_ints, c_occ, c_vir, eps_occ, eps_vir):
        vm = pl.BlockSpec(memory_space=pltpu.VMEM)
        e = pl.pallas_call(
            kernel,
            out_shape=pltpu.VMEM((OD, O), F32),
            in_specs=[pl.BlockSpec(memory_space=pltpu.HBM)] * 5,
            out_specs=vm,
            scratch_shapes=[
                pltpu.VMEM((O, N), BF16),
                pltpu.VMEM((V, N), BF16),
                pltpu.SMEM((O,), F32),
                pltpu.VMEM((1, V), F32),
                pltpu.VMEM((SLOTS, N, N, N), BF16),
                pltpu.VMEM((2 * O, 2 * N), BF16),
                pltpu.VMEM((OD * L, JB), BF16),
                pltpu.VMEM((GR, PC * N), BF16),
                pltpu.VMEM((8 * O, 2 * NC * 16), BF16),
                pltpu.VMEM((8 * O, 2 * NC * 16), BF16),
                pltpu.VMEM((N * O, L), F32),
                pltpu.VMEM((N * O, L), F32),
                pltpu.VMEM((NDEV, PC * N, JB), BF16),
                pltpu.VMEM((NC, 3, GR, JB), BF16),
                pltpu.VMEM((NC, GR, JB), BF16),
                pltpu.VMEM((NC, GR, JB), BF16),
                pltpu.VMEM((2, NC, GH, JB), BF16),
                pltpu.VMEM((NC, XR, JB), BF16),
                pltpu.VMEM((IG, 3, VR, L), F32),
                pltpu.VMEM((IG, 3, VR, L), F32),
                pltpu.VMEM((IG, 3, AO * 16, L), F32),
                pltpu.VMEM((O * OD, 80, L), F32),
                pltpu.VMEM((OD, O * 8, L), F32),
                pltpu.SemaphoreType.DMA((SLOTS,)),
                pltpu.SemaphoreType.DMA((4,)),
                pltpu.SemaphoreType.DMA((NC, 4)),
                pltpu.SemaphoreType.DMA((2, NC)),
                pltpu.SemaphoreType.DMA((NC,)),
                pltpu.SemaphoreType.DMA((NC,)),
                pltpu.SemaphoreType.DMA((IG,)),
                pltpu.SemaphoreType.DMA((IG,)),
            ],
            compiler_params=pltpu.CompilerParams(
                collective_id=0, has_side_effects=True, vmem_limit_bytes=60 * 2**20),
        )(a_ints, c_occ.T, c_vir.T, eps_occ, eps_vir.reshape(1, V))
        return e.T

    return jax.shard_map(
        per_device,
        mesh=mesh,
        in_specs=(P(("frag", "dev")), P("frag"), P("frag"), P("frag"), P("frag")),
        out_specs=P("frag", "dev"),
        check_vma=False,
    )
```

```python
import functools

import jax
import jax.numpy as jnp
from jax import lax
from jax.experimental import pallas as pl
from jax.experimental.pallas import tpu as pltpu
from jax.sharding import PartitionSpec as P

MESH = pl.DeviceIdType.MESH
F32, BF16 = jnp.float32, jnp.bfloat16

N = 96
O = 20
V = 75
NDEV = 4
NP = N // NDEV
OD = O // NDEV
L = 128
JB = 384
PC = 2
NC = NP // PC
AO = 10
GR = AO * 8 * PC
AV = 76
SLOTS = 6
A1 = 28
U0 = A1 // 8
U2 = -(-A1 // 16)
PH = U2 * 16
XR = GR - U0 * 16
VT = (V - A1) * 2
VO = (A1 - U0 * 8) * 2
VR = -(-VT // 8) * 8
FK = NP * 16
IG = O // 2


def _dot(x, y):
    return jnp.dot(x, y, preferred_element_type=F32)


def _div(x, d):
    return jnp.floor((x + 0.5) * (1.0 / d))


def _rows(shape):
    return lax.broadcasted_iota(jnp.int32, shape, 0).astype(F32)


def _cols(shape):
    return lax.broadcasted_iota(jnp.int32, shape, 1).astype(F32)


def _onehot(cond):
    return jnp.where(cond, 1.0, 0.0).astype(BF16)


def _spread(m, row_of, col_of, keep, shape):
    r_shape, c_shape = (shape[0], m.shape[0]), (m.shape[1], shape[1])
    left = _onehot(row_of(_rows(r_shape)) == _cols(r_shape))
    right = _onehot(_rows(c_shape) == col_of(_cols(c_shape)))
    full = _dot(_dot(left, m).astype(BF16), right)
    return jnp.where(keep(_rows(shape), _cols(shape)), full, 0.0).astype(BF16)


def kernel(a_hbm, co_hbm, cv_hbm, eo_hbm, ev_hbm, out_ref, co_ref, cv_ref, eo_ref, ev_ref, a_buf, l1, w2, l3, lp, l4, l4f,
           t0_s, t1_s, h_s, g_send, g_own, g_near, p_send, p_far, x_near, v_send, v_recv, v_s, r_s, e_s,
           a_sem, in_sem, send_sem, ps_sem, pf_sem, near_sem, x_sem, vs_sem, vr_sem):
    f, me = lax.axis_index("frag"), lax.axis_index("dev")
    chip, core = me // 2, lax.rem(me, 2)
    far0 = (1 - chip) * 2 + core
    far1 = (1 - chip) * 2 + 1 - core
    near = chip * 2 + 1 - core
    peers = (far0, far1, near)

    def a_copy(p, slot):
        return pltpu.make_async_copy(a_hbm.at[p], a_buf.at[slot], a_sem.at[slot])

    if PH > A1:
        p_far[:, :, :, PH - 16:, :] = jnp.zeros((2, NP, 3, 16, L), BF16)
    barrier = pltpu.get_barrier_semaphore()
    for d in peers:
        pl.semaphore_signal(barrier, inc=1, device_id=(f, d), device_id_type=MESH)
    small = [pltpu.make_async_copy(x, y, in_sem.at[k]) for k, (x, y) in enumerate(
        [(co_hbm, co_ref), (cv_hbm, cv_ref), (eo_hbm, eo_ref), (ev_hbm, ev_ref)])]
    for cp in small[:2]:
        cp.start()
    a_copy(0, 0).start()
    for cp in small[:2]:
        cp.wait()
    for s in range(1, SLOTS):
        a_copy(s, s).start()
    for cp in small[2:]:
        cp.start()

    co, cv = co_ref[...], cv_ref[...]
    mod = lambda x, d: x - d * _div(x, d)
    co_pad = jnp.pad(co.astype(F32), ((0, O), (0, 256 - N)))
    l1[...] = (co_pad + pltpu.roll(pltpu.roll(co_pad, O, axis=0), N, axis=1)).astype(BF16)[:, :2 * N]
    cv_t = jnp.pad(cv.astype(F32), ((0, L - V), (0, L - N))).T
    cv_pad = jnp.pad(cv_t, ((0, 0), (0, JB - L)))
    for jj in range(OD):
        w2[jj * L:(jj + 1) * L, :] = (pltpu.roll(cv_pad, V * jj, axis=1) if jj else cv_pad).astype(BF16)
    lp[...] = cv[:PH]

    def build_l3():
        twice = _dot(_onehot(_div(_rows((GR, V)), PC) == _cols((GR, V))), cv)
        twice = jnp.pad(twice, ((0, 0), (0, 256 - N)))
        l3[...] = jnp.where(mod(_rows((GR, 256)), PC) == 0, twice, pltpu.roll(twice, N, axis=1)).astype(BF16)[:, :PC * N]

    def spread_co(slot0, slot1):
        return _spread(
            co, lambda x: _div(x, 16) * 2 + mod(x, 2),
            lambda y: jnp.where(y < NC * 16, slot0, slot1).astype(F32) * NP + _div(mod(y, NC * 16), 16) * PC + mod(y, PC),
            lambda x, y: _div(mod(x, 16), 2) == _div(mod(y, 16), PC), (8 * O, 2 * NC * 16))

    def p_copy(p, k):
        return pltpu.make_async_remote_copy(
            src_ref=p_send.at[p, k, :, pl.ds(0, A1)], dst_ref=p_far.at[k, p, :, pl.ds(0, A1)], send_sem=ps_sem.at[p, k],
            recv_sem=pf_sem.at[k, p], device_id=(f, peers[k]), device_id_type=MESH)

    def x_copy(c):
        return pltpu.make_async_remote_copy(
            src_ref=g_send.at[c, 1, pl.ds(U0 * 16, XR)], dst_ref=x_near.at[c], send_sem=send_sem.at[c, 0],
            recv_sem=x_sem.at[c], device_id=(f, near), device_id_type=MESH)

    def n_copy(c):
        return pltpu.make_async_remote_copy(
            src_ref=g_send.at[c, 2], dst_ref=g_near.at[c], send_sem=send_sem.at[c, 1],
            recv_sem=near_sem.at[c], device_id=(f, near), device_id_type=MESH)

    def v_copy(g):
        return pltpu.make_async_remote_copy(
            src_ref=v_send.at[g, :, pl.ds(0, VT)], dst_ref=v_recv.at[g, :, pl.ds(0, VT)], send_sem=vs_sem.at[g],
            recv_sem=vr_sem.at[g], device_id=(f, far0), device_id_type=MESH)

    def first_step(slot, buf, q):
        x0 = jnp.pad(a_buf[slot, q:q + 2].reshape(2 * N, N), ((0, 0), (0, L - N)))
        x1 = jnp.pad(a_buf[slot, q + 2:q + 4].reshape(2 * N, N), ((0, 0), (0, L - N)))
        t = _dot(l1[...], jnp.concatenate([x0, x1], axis=1))
        buf[q * O:(q + 2) * O, :] = t[:, :L]
        buf[(q + 2) * O:(q + 4) * O, :] = t[:, L:]

    def second_step(buf, row):
        x = [jnp.concatenate([buf[pl.ds(d * OD + jj, N, stride=O), :].astype(BF16) for d in range(NDEV)], axis=0)
             for jj in range(OD)]
        h0 = _dot(jnp.concatenate(x[:4], axis=1), w2[:4 * L, :256]).astype(BF16)
        h1 = _dot(jnp.concatenate(x[2:], axis=1), w2[2 * L:, 256:]).astype(BF16)
        for d in range(NDEV):
            h_s[d, row * N:(row + 1) * N, :256] = h0[d * N:(d + 1) * N]
            h_s[d, row * N:(row + 1) * N, 256:] = h1[d * N:(d + 1) * N]

    def piece(p, row):
        for k in range(2):
            g = _dot(lp[...], h_s[peers[k], row * N:(row + 1) * N, :]).astype(BF16)
            for n in range(3):
                p_send[p, k, n] = g[:, n * L:(n + 1) * L]

    def third_step(c, k):
        r0 = U0 * 16 if k < 2 else 0
        g = _dot(l3[r0:, :], h_s[(far0, far1, near, me)[k]]).astype(BF16)
        if k < 3:
            g_send[c, k, r0:, :] = g
        else:
            g_own[c] = g

    def prefetch(p, slot):
        @pl.when(p + SLOTS < NP)
        def _():
            a_copy(p + SLOTS, slot).start()
            a_copy(p + 1 + SLOTS, slot + 1).start()

    def send_piece(p):
        p_copy(p, 0).start()
        p_copy(p, 1).start()

    a_copy(0, 0).wait()
    for q in range(0, N, 4):
        first_step(0, t0_s, q)
    second_step(t0_s, 0)
    piece(0, 0)
    pl.semaphore_wait(barrier, 3)
    send_piece(0)
    a_copy(1, 1).wait()
    for q in range(0, N, 4):
        first_step(1, t1_s, q)
    build_l3()
    prefetch(0, 0)

    def chunk(c, _):
        p = c * PC
        slot = lax.rem(p, SLOTS)
        a_copy(p, slot).wait()
        for n, q in enumerate(range(0, N, 4)):
            if n == 1:
                second_step(t1_s, 1)
            first_step(slot, t0_s, q)
            if n == 8:
                piece(p - 1, 1)
            if n in (11, 14, 17, 20):
                third_step(c - 1, (n - 11) // 3)
        send_piece(p - 1)
        x_copy(c - 1).start()
        n_copy(c - 1).start()
        a_copy(p + 1, slot + 1).wait()
        for n, q in enumerate(range(0, N, 4)):
            if n == 1:
                second_step(t0_s, 0)
            first_step(slot + 1, t1_s, q)
            if n == 12:
                piece(p, 0)
        send_piece(p)
        prefetch(p, slot)
        return 0

    lax.fori_loop(1, NC, chunk, 0)
    last = NC - 1
    second_step(t1_s, 1)
    third_step(last, 1)
    third_step(last, 0)
    piece(NP - 1, 1)
    x_copy(last).start()
    send_piece(NP - 1)
    third_step(last, 2)
    n_copy(last).start()
    third_step(last, 3)

    l4[...] = spread_co(me, near)

    def octet(own, other, t, t_other):
        rows = pl.ds(pl.multiple_of(t * 16, 16), 16)
        orows = pl.ds(pl.multiple_of(t_other * 16, 16), 16)
        return jnp.concatenate([own[:, rows].reshape(NC * 16, JB), other[:, orows].reshape(NC * 16, JB)], axis=0)

    for c in range(NC):
        x_copy(c).wait_recv()

    def partial(t):
        v = _dot(l4[...], octet(g_send.at[:, 0], x_near, t, t - U0))
        r0 = VO if t == U0 else 0
        r1 = min(16, V * 2 - t * 16)
        at = t * 16 - A1 * 2
        for g in range(IG):
            for n in range(3):
                v_send[g, n, at + r0:at + r1, :] = v[g * 16 + r0:g * 16 + r1, n * L:(n + 1) * L]

    for t in range(U0, AO):
        partial(t)
    for g in range(IG):
        v_copy(g).start()

    l4f[...] = _spread(
        co, lambda x: _div(x, 32) * 2 + mod(x, 2),
        lambda y: jnp.where(y < FK, far0, far1).astype(F32) * NP + _div(mod(y, FK), 16),
        lambda x, y: _div(mod(x, 32), 2) == mod(y, 16), (16 * O, 2 * FK))

    for cp in small[2:]:
        cp.wait()
    ev = jnp.broadcast_to(ev_ref[...], (L, V))
    ev = jnp.pad(ev, ((0, 0), (0, L - V)))
    pair = ev + ev.T
    inside = (_rows((80, L)) < V) & (_cols((80, L)) < V)

    def recip(i, _):
        for jj in range(OD):
            den = (eo_ref[i] + eo_ref[me * OD + jj]) - pair[:80]
            r_s[i * OD + jj] = jnp.where(inside, 1.0 / den, 0.0)
        return 0

    lax.fori_loop(0, O, recip, 0)

    for c in range(NC):
        n_copy(c).wait_recv()

    def contract(t, _):
        v = _dot(l4[...], octet(g_own, g_near, t, t))
        rows = pl.ds(pl.multiple_of(t * 16, 16), 16)
        for g in range(IG):
            for n in range(3):
                v_s[g, n, rows, :] = v[g * 16:(g + 1) * 16, n * L:(n + 1) * L]
        return 0

    lax.fori_loop(0, AO, contract, 0)
    for p in range(NP):
        for k in range(2):
            p_copy(p, k).wait_recv()

    for u in range(U2):
        for n in range(3):
            v = _dot(l4f[...], p_far[:, :, n, u * 16:(u + 1) * 16, :].reshape(2 * FK, L))
            for g in range(IG):
                v_s[g, n, u * 32:(u + 1) * 32, :] += v[g * 32:(g + 1) * 32]

    def energy(g, _):
        v_copy(g).wait_recv()
        v_s[g, :, A1 * 2:V * 2, :] += v_recv[g, :, :VT]
        lane = lax.broadcasted_iota(jnp.int32, (80, L), 1)
        for ii in range(2):
            i = g * 2 + ii
            tiles = [v_s[g, n, pl.ds(ii, 80, stride=2), :] for n in range(3)]
            for jj in range(OD):
                t, off = divmod(V * jj, L)
                m = pltpu.roll(tiles[t], (L - off) % L, axis=1) if off else tiles[t]
                if off + V > L:
                    m = jnp.where(lane < L - off, m, pltpu.roll(tiles[t + 1], L - off, axis=1))
                mt = jnp.pad(m, ((0, L - 80), (0, 0))).T[:80]
                term = m * (2.0 * m - mt) * r_s[i * OD + jj]
                e_s[jj, pl.ds(pl.multiple_of(i * 8, 8), 8), :] = jnp.sum(term.reshape(10, 8, L), axis=0)
        return 0

    lax.fori_loop(0, IG, energy, 0)
    for jj in range(OD):
        tot = e_s[jj, pl.ds(0, O, stride=8), :]
        for s in range(1, 8):
            tot = tot + e_s[jj, pl.ds(s, O, stride=8), :]
        col = jnp.sum(jnp.pad(tot, ((0, 32 - O), (0, 0))).T, axis=0, keepdims=True)
        out_ref[jj:jj + 1, :] = col[:, :O]

    for p in range(NP):
        p_copy(p, 0).wait_send()
        p_copy(p, 1).wait_send()
    for c in range(NC):
        x_copy(c).wait_send()
        n_copy(c).wait_send()
    for g in range(IG):
        v_copy(g).wait_send()


def solution(mesh):
    def per_device(a_ints, c_occ, c_vir, eps_occ, eps_vir):
        vm = pl.BlockSpec(memory_space=pltpu.VMEM)
        e = pl.pallas_call(
            kernel,
            out_shape=pltpu.VMEM((OD, O), F32),
            in_specs=[pl.BlockSpec(memory_space=pltpu.HBM)] * 5,
            out_specs=vm,
            scratch_shapes=[
                pltpu.VMEM((O, N), BF16),
                pltpu.VMEM((V, N), BF16),
                pltpu.SMEM((O,), F32),
                pltpu.VMEM((1, V), F32),
                pltpu.VMEM((SLOTS, N, N, N), BF16),
                pltpu.VMEM((2 * O, 2 * N), BF16),
                pltpu.VMEM((OD * L, JB), BF16),
                pltpu.VMEM((GR, PC * N), BF16),
                pltpu.VMEM((PH, N), BF16),
                pltpu.VMEM((8 * O, 2 * NC * 16), BF16),
                pltpu.VMEM((16 * O, 2 * FK), BF16),
                pltpu.VMEM((N * O, L), F32),
                pltpu.VMEM((N * O, L), F32),
                pltpu.VMEM((NDEV, PC * N, JB), BF16),
                pltpu.VMEM((NC, 3, GR, JB), BF16),
                pltpu.VMEM((NC, GR, JB), BF16),
                pltpu.VMEM((NC, GR, JB), BF16),
                pltpu.VMEM((NP, 2, 3, PH, L), BF16),
                pltpu.VMEM((2, NP, 3, PH, L), BF16),
                pltpu.VMEM((NC, XR, JB), BF16),
                pltpu.VMEM((IG, 3, VR, L), F32),
                pltpu.VMEM((IG, 3, VR, L), F32),
                pltpu.VMEM((IG, 3, AO * 16, L), F32),
                pltpu.VMEM((O * OD, 80, L), F32),
                pltpu.VMEM((OD, O * 8, L), F32),
                pltpu.SemaphoreType.DMA((SLOTS,)),
                pltpu.SemaphoreType.DMA((4,)),
                pltpu.SemaphoreType.DMA((NC, 2)),
                pltpu.SemaphoreType.DMA((NP, 2)),
                pltpu.SemaphoreType.DMA((2, NP)),
                pltpu.SemaphoreType.DMA((NC,)),
                pltpu.SemaphoreType.DMA((NC,)),
                pltpu.SemaphoreType.DMA((IG,)),
                pltpu.SemaphoreType.DMA((IG,)),
            ],
            compiler_params=pltpu.CompilerParams(
                collective_id=0, has_side_effects=True, vmem_limit_bytes=60 * 2**20),
        )(a_ints, c_occ.T, c_vir.T, eps_occ, eps_vir.reshape(1, V))
        return e.T

    return jax.shard_map(
        per_device,
        mesh=mesh,
        in_specs=(P(("frag", "dev")), P("frag"), P("frag"), P("frag"), P("frag")),
        out_specs=P("frag", "dev"),
        check_vma=False,
    )
```

```python
import functools

import jax
import jax.numpy as jnp
from jax import lax
from jax.experimental import pallas as pl
from jax.experimental.pallas import tpu as pltpu
from jax.sharding import PartitionSpec as P

MESH = pl.DeviceIdType.MESH
F32, BF16 = jnp.float32, jnp.bfloat16

N = 96
O = 20
V = 75
NDEV = 4
NP = N // NDEV
OD = O // NDEV
L = 128
JB = 384
PC = 2
NC = NP // PC
AO = 10
GR = AO * 8 * PC
AV = 76
SLOTS = 6
A1 = 26
U0 = A1 // 8
U2 = -(-A1 // 16)
PH = U2 * 16
XR = GR - U0 * 16
VT = (V - A1) * 2
VO = (A1 - U0 * 8) * 2
VR = -(-VT // 8) * 8
FK = NP * 16
IG = O // 2


def _dot(x, y):
    return jnp.dot(x, y, preferred_element_type=F32)


def _div(x, d):
    return jnp.floor((x + 0.5) * (1.0 / d))


def _rows(shape):
    return lax.broadcasted_iota(jnp.int32, shape, 0).astype(F32)


def _cols(shape):
    return lax.broadcasted_iota(jnp.int32, shape, 1).astype(F32)


def _onehot(cond):
    return jnp.where(cond, 1.0, 0.0).astype(BF16)


def _spread(m, row_of, col_of, keep, shape):
    r_shape, c_shape = (shape[0], m.shape[0]), (m.shape[1], shape[1])
    left = _onehot(row_of(_rows(r_shape)) == _cols(r_shape))
    right = _onehot(_rows(c_shape) == col_of(_cols(c_shape)))
    full = _dot(_dot(left, m).astype(BF16), right)
    return jnp.where(keep(_rows(shape), _cols(shape)), full, 0.0).astype(BF16)


def kernel(a_hbm, co_hbm, cv_hbm, eo_hbm, ev_hbm, out_ref, co_ref, cv_ref, eo_ref, ev_ref, a_buf, l1, w2, l3, lp, l4, l4f,
           t0_s, t1_s, h_s, g_send, g_own, g_near, p_send, p_far, x_near, v_send, v_recv, v_s, r_s, e_s,
           a_sem, in_sem, send_sem, ps_sem, pf_sem, near_sem, x_sem, vs_sem, vr_sem):
    f, me = lax.axis_index("frag"), lax.axis_index("dev")
    chip, core = me // 2, lax.rem(me, 2)
    far0 = (1 - chip) * 2 + core
    far1 = (1 - chip) * 2 + 1 - core
    near = chip * 2 + 1 - core
    peers = (far0, far1, near)

    def a_copy(p, slot):
        return pltpu.make_async_copy(a_hbm.at[p], a_buf.at[slot], a_sem.at[slot])

    small = [pltpu.make_async_copy(x, y, in_sem.at[k]) for k, (x, y) in enumerate(
        [(co_hbm, co_ref), (cv_hbm, cv_ref), (eo_hbm, eo_ref), (ev_hbm, ev_ref)])]
    for cp in small[:2]:
        cp.start()
    a_copy(0, 0).start()
    if PH > A1:
        p_far[:, :, :, PH - 16:, :] = jnp.zeros((2, NP, 3, 16, L), BF16)
    barrier = pltpu.get_barrier_semaphore()
    for d in peers:
        pl.semaphore_signal(barrier, inc=1, device_id=(f, d), device_id_type=MESH)
    for cp in small[:2]:
        cp.wait()
    for s in range(1, SLOTS):
        a_copy(s, s).start()
    for cp in small[2:]:
        cp.start()

    co, cv = co_ref[...], cv_ref[...]
    mod = lambda x, d: x - d * _div(x, d)
    co_pad = jnp.pad(co.astype(F32), ((0, O), (0, 256 - N)))
    l1[...] = (co_pad + pltpu.roll(pltpu.roll(co_pad, O, axis=0), N, axis=1)).astype(BF16)[:, :2 * N]
    cv_t = jnp.pad(cv.astype(F32), ((0, L - V), (0, L - N))).T
    cv_pad = jnp.pad(cv_t, ((0, 0), (0, JB - L)))
    for jj in range(OD):
        w2[jj * L:(jj + 1) * L, :] = (pltpu.roll(cv_pad, V * jj, axis=1) if jj else cv_pad).astype(BF16)
    lp[...] = cv[:PH]

    def build_l3():
        twice = _dot(_onehot(_div(_rows((GR, V)), PC) == _cols((GR, V))), cv)
        twice = jnp.pad(twice, ((0, 0), (0, 256 - N)))
        l3[...] = jnp.where(mod(_rows((GR, 256)), PC) == 0, twice, pltpu.roll(twice, N, axis=1)).astype(BF16)[:, :PC * N]

    def spread_co(slot0, slot1):
        return _spread(
            co, lambda x: _div(x, 16) * 2 + mod(x, 2),
            lambda y: jnp.where(y < NC * 16, slot0, slot1).astype(F32) * NP + _div(mod(y, NC * 16), 16) * PC + mod(y, PC),
            lambda x, y: _div(mod(x, 16), 2) == _div(mod(y, 16), PC), (8 * O, 2 * NC * 16))

    def p_copy(p, k):
        return pltpu.make_async_remote_copy(
            src_ref=p_send.at[p, k, :, pl.ds(0, A1)], dst_ref=p_far.at[k, p, :, pl.ds(0, A1)], send_sem=ps_sem.at[p, k],
            recv_sem=pf_sem.at[k, p], device_id=(f, peers[k]), device_id_type=MESH)

    def x_copy(c):
        return pltpu.make_async_remote_copy(
            src_ref=g_send.at[c, 1, pl.ds(U0 * 16, XR)], dst_ref=x_near.at[c], send_sem=send_sem.at[c, 0],
            recv_sem=x_sem.at[c], device_id=(f, near), device_id_type=MESH)

    def n_copy(c):
        return pltpu.make_async_remote_copy(
            src_ref=g_send.at[c, 2], dst_ref=g_near.at[c], send_sem=send_sem.at[c, 1],
            recv_sem=near_sem.at[c], device_id=(f, near), device_id_type=MESH)

    def v_copy(g):
        return pltpu.make_async_remote_copy(
            src_ref=v_send.at[g, :, pl.ds(0, VT)], dst_ref=v_recv.at[g, :, pl.ds(0, VT)], send_sem=vs_sem.at[g],
            recv_sem=vr_sem.at[g], device_id=(f, far0), device_id_type=MESH)

    def first_step(slot, buf, q):
        x0 = jnp.pad(a_buf[slot, q:q + 2].reshape(2 * N, N), ((0, 0), (0, L - N)))
        x1 = jnp.pad(a_buf[slot, q + 2:q + 4].reshape(2 * N, N), ((0, 0), (0, L - N)))
        t = _dot(l1[...], jnp.concatenate([x0, x1], axis=1))
        buf[q * O:(q + 2) * O, :] = t[:, :L]
        buf[(q + 2) * O:(q + 4) * O, :] = t[:, L:]

    def second_step(buf, row):
        x = [jnp.concatenate([buf[pl.ds(d * OD + jj, N, stride=O), :].astype(BF16) for d in range(NDEV)], axis=0)
             for jj in range(OD)]
        h0 = _dot(jnp.concatenate(x[:4], axis=1), w2[:4 * L, :256]).astype(BF16)
        h1 = _dot(jnp.concatenate(x[2:], axis=1), w2[2 * L:, 256:]).astype(BF16)
        for d in range(NDEV):
            h_s[d, row * N:(row + 1) * N, :256] = h0[d * N:(d + 1) * N]
            h_s[d, row * N:(row + 1) * N, 256:] = h1[d * N:(d + 1) * N]

    def piece(p, row):
        for k in range(2):
            g = _dot(lp[...], h_s[peers[k], row * N:(row + 1) * N, :]).astype(BF16)
            for n in range(3):
                p_send[p, k, n] = g[:, n * L:(n + 1) * L]

    def third_step(c, k):
        r0 = U0 * 16 if k < 2 else 0
        g = _dot(l3[r0:, :], h_s[(far0, far1, near, me)[k]]).astype(BF16)
        if k < 3:
            g_send[c, k, r0:, :] = g
        else:
            g_own[c] = g

    def prefetch(p, slot):
        @pl.when(p + SLOTS < NP)
        def _():
            a_copy(p + SLOTS, slot).start()
            a_copy(p + 1 + SLOTS, slot + 1).start()

    def send_piece(p):
        p_copy(p, 0).start()
        p_copy(p, 1).start()

    a_copy(0, 0).wait()
    for q in range(0, N, 4):
        first_step(0, t0_s, q)
    second_step(t0_s, 0)
    piece(0, 0)
    pl.semaphore_wait(barrier, 3)
    send_piece(0)
    a_copy(1, 1).wait()
    for q in range(0, N, 4):
        first_step(1, t1_s, q)
    build_l3()
    prefetch(0, 0)

    def chunk(c, _):
        p = c * PC
        slot = lax.rem(p, SLOTS)
        a_copy(p, slot).wait()
        for n, q in enumerate(range(0, N, 4)):
            if n == 1:
                second_step(t1_s, 1)
            first_step(slot, t0_s, q)
            if n == 8:
                piece(p - 1, 1)
            if n in (11, 14, 17, 20):
                third_step(c - 1, (n - 11) // 3)
        x_copy(c - 1).start()
        send_piece(p - 1)
        a_copy(p + 1, slot + 1).wait()
        for n, q in enumerate(range(0, N, 4)):
            if n == 1:
                second_step(t0_s, 0)
            first_step(slot + 1, t1_s, q)
            if n == 12:
                piece(p, 0)
        send_piece(p)
        prefetch(p, slot)
        return 0

    lax.fori_loop(1, NC, chunk, 0)
    last = NC - 1
    second_step(t1_s, 1)
    third_step(last, 1)
    x_copy(last).start()
    third_step(last, 0)
    piece(NP - 1, 1)
    send_piece(NP - 1)
    third_step(last, 2)
    third_step(last, 3)

    l4[...] = spread_co(me, near)

    def octet(own, other, t, t_other):
        rows = pl.ds(pl.multiple_of(t * 16, 16), 16)
        orows = pl.ds(pl.multiple_of(t_other * 16, 16), 16)
        return jnp.concatenate([own[:, rows].reshape(NC * 16, JB), other[:, orows].reshape(NC * 16, JB)], axis=0)

    for c in range(NC):
        x_copy(c).wait_recv()

    def partial(t):
        v = _dot(l4[...], octet(g_send.at[:, 0], x_near, t, t - U0))
        r0 = VO if t == U0 else 0
        r1 = min(16, V * 2 - t * 16)
        at = t * 16 - A1 * 2
        for g in range(IG):
            for n in range(3):
                v_send[g, n, at + r0:at + r1, :] = v[g * 16 + r0:g * 16 + r1, n * L:(n + 1) * L]

    for t in range(U0, AO):
        partial(t)
    for g in range(IG):
        v_copy(g).start()
    for c in range(NC):
        n_copy(c).start()

    l4f[...] = _spread(
        co, lambda x: _div(x, 32) * 2 + mod(x, 2),
        lambda y: jnp.where(y < FK, far0, far1).astype(F32) * NP + _div(mod(y, FK), 16),
        lambda x, y: _div(mod(x, 32), 2) == mod(y, 16), (16 * O, 2 * FK))

    for cp in small[2:]:
        cp.wait()
    ev = jnp.broadcast_to(ev_ref[...], (L, V))
    ev = jnp.pad(ev, ((0, 0), (0, L - V)))
    pair = ev + ev.T
    inside = (_rows((80, L)) < V) & (_cols((80, L)) < V)

    def recip(i, _):
        for jj in range(OD):
            den = (eo_ref[i] + eo_ref[me * OD + jj]) - pair[:80]
            r_s[i * OD + jj] = jnp.where(inside, 1.0 / den, 0.0)
        return 0

    lax.fori_loop(0, O, recip, 0)

    for c in range(NC):
        n_copy(c).wait_recv()

    def contract(t, _):
        v = _dot(l4[...], octet(g_own, g_near, t, t))
        rows = pl.ds(pl.multiple_of(t * 16, 16), 16)
        for g in range(IG):
            for n in range(3):
                v_s[g, n, rows, :] = v[g * 16:(g + 1) * 16, n * L:(n + 1) * L]
        return 0

    lax.fori_loop(0, AO, contract, 0)
    for p in range(NP):
        for k in range(2):
            p_copy(p, k).wait_recv()

    for u in range(U2):
        for n in range(3):
            v = _dot(l4f[...], p_far[:, :, n, u * 16:(u + 1) * 16, :].reshape(2 * FK, L))
            for g in range(IG):
                v_s[g, n, u * 32:(u + 1) * 32, :] += v[g * 32:(g + 1) * 32]

    for p in range(NP):
        p_copy(p, 0).wait_send()
        p_copy(p, 1).wait_send()
    for c in range(NC):
        x_copy(c).wait_send()
        n_copy(c).wait_send()
    def energy(g, _):
        v_copy(g).wait()
        v_s[g, :, A1 * 2:V * 2, :] += v_recv[g, :, :VT]
        lane = lax.broadcasted_iota(jnp.int32, (80, L), 1)
        for ii in range(2):
            i = g * 2 + ii
            tiles = [v_s[g, n, pl.ds(ii, 80, stride=2), :] for n in range(3)]
            for jj in range(OD):
                t, off = divmod(V * jj, L)
                m = pltpu.roll(tiles[t], (L - off) % L, axis=1) if off else tiles[t]
                if off + V > L:
                    m = jnp.where(lane < L - off, m, pltpu.roll(tiles[t + 1], L - off, axis=1))
                mt = jnp.pad(m, ((0, L - 80), (0, 0))).T[:80]
                term = m * (2.0 * m - mt) * r_s[i * OD + jj]
                e_s[jj, pl.ds(pl.multiple_of(i * 8, 8), 8), :] = jnp.sum(term.reshape(10, 8, L), axis=0)
        return 0

    lax.fori_loop(0, IG, energy, 0)
    for jj in range(OD):
        tot = e_s[jj, pl.ds(0, O, stride=8), :]
        for s in range(1, 8):
            tot = tot + e_s[jj, pl.ds(s, O, stride=8), :]
        col = jnp.sum(jnp.pad(tot, ((0, 32 - O), (0, 0))).T, axis=0, keepdims=True)
        out_ref[jj:jj + 1, :] = col[:, :O]


def solution(mesh):
    def per_device(a_ints, c_occ, c_vir, eps_occ, eps_vir):
        vm = pl.BlockSpec(memory_space=pltpu.VMEM)
        e = pl.pallas_call(
            kernel,
            out_shape=pltpu.VMEM((OD, O), F32),
            in_specs=[pl.BlockSpec(memory_space=pltpu.HBM)] * 5,
            out_specs=vm,
            scratch_shapes=[
                pltpu.VMEM((O, N), BF16),
                pltpu.VMEM((V, N), BF16),
                pltpu.SMEM((O,), F32),
                pltpu.VMEM((1, V), F32),
                pltpu.VMEM((SLOTS, N, N, N), BF16),
                pltpu.VMEM((2 * O, 2 * N), BF16),
                pltpu.VMEM((OD * L, JB), BF16),
                pltpu.VMEM((GR, PC * N), BF16),
                pltpu.VMEM((PH, N), BF16),
                pltpu.VMEM((8 * O, 2 * NC * 16), BF16),
                pltpu.VMEM((16 * O, 2 * FK), BF16),
                pltpu.VMEM((N * O, L), F32),
                pltpu.VMEM((N * O, L), F32),
                pltpu.VMEM((NDEV, PC * N, JB), BF16),
                pltpu.VMEM((NC, 3, GR, JB), BF16),
                pltpu.VMEM((NC, GR, JB), BF16),
                pltpu.VMEM((NC, GR, JB), BF16),
                pltpu.VMEM((NP, 2, 3, PH, L), BF16),
                pltpu.VMEM((2, NP, 3, PH, L), BF16),
                pltpu.VMEM((NC, XR, JB), BF16),
                pltpu.VMEM((IG, 3, VR, L), F32),
                pltpu.VMEM((IG, 3, VR, L), F32),
                pltpu.VMEM((IG, 3, AO * 16, L), F32),
                pltpu.VMEM((O * OD, 80, L), F32),
                pltpu.VMEM((OD, O * 8, L), F32),
                pltpu.SemaphoreType.DMA((SLOTS,)),
                pltpu.SemaphoreType.DMA((4,)),
                pltpu.SemaphoreType.DMA((NC, 2)),
                pltpu.SemaphoreType.DMA((NP, 2)),
                pltpu.SemaphoreType.DMA((2, NP)),
                pltpu.SemaphoreType.DMA((NC,)),
                pltpu.SemaphoreType.DMA((NC,)),
                pltpu.SemaphoreType.DMA((IG,)),
                pltpu.SemaphoreType.DMA((IG,)),
            ],
            compiler_params=pltpu.CompilerParams(
                collective_id=0, has_side_effects=True, vmem_limit_bytes=60 * 2**20),
        )(a_ints, c_occ.T, c_vir.T, eps_occ, eps_vir.reshape(1, V))
        return e.T

    return jax.shard_map(
        per_device,
        mesh=mesh,
        in_specs=(P(("frag", "dev")), P("frag"), P("frag"), P("frag"), P("frag")),
        out_specs=P("frag", "dev"),
        check_vma=False,
    )
```

```python
import functools

import jax
import jax.numpy as jnp
from jax import lax
from jax.experimental import pallas as pl
from jax.experimental.pallas import tpu as pltpu
from jax.sharding import PartitionSpec as P

MESH = pl.DeviceIdType.MESH
F32, BF16 = jnp.float32, jnp.bfloat16

N = 96
O = 20
V = 75
NDEV = 4
NP = N // NDEV
OD = O // NDEV
L = 128
JB = 384
PC = 2
NC = NP // PC
AO = 10
GR = AO * 8 * PC
AV = 76
SLOTS = 6
A1 = 26
U0 = A1 // 8
U2 = -(-A1 // 16)
PH = U2 * 16
XR = GR - U0 * 16
VT = (V - A1) * 2
VO = (A1 - U0 * 8) * 2
VR = -(-VT // 8) * 8
FK = NP * 16
IG = O // 2


def _dot(x, y):
    return jnp.dot(x, y, preferred_element_type=F32)


def _div(x, d):
    return jnp.floor((x + 0.5) * (1.0 / d))


def _rows(shape):
    return lax.broadcasted_iota(jnp.int32, shape, 0).astype(F32)


def _cols(shape):
    return lax.broadcasted_iota(jnp.int32, shape, 1).astype(F32)


def _onehot(cond):
    return jnp.where(cond, 1.0, 0.0).astype(BF16)


def _spread(m, row_of, col_of, keep, shape):
    r_shape, c_shape = (shape[0], m.shape[0]), (m.shape[1], shape[1])
    left = _onehot(row_of(_rows(r_shape)) == _cols(r_shape))
    right = _onehot(_rows(c_shape) == col_of(_cols(c_shape)))
    full = _dot(_dot(left, m).astype(BF16), right)
    return jnp.where(keep(_rows(shape), _cols(shape)), full, 0.0).astype(BF16)


def kernel(a_hbm, co_hbm, cv_hbm, eo_hbm, ev_hbm, out_ref, co_ref, cv_ref, eo_ref, ev_ref, a_buf, l1, w2, l3, lp, l4, l4f,
           t0_s, t1_s, h_s, g_send, g_own, g_near, p_send, p_far, x_near, v_send, v_recv, v_s, r_s, e_s,
           a_sem, in_sem, send_sem, ps_sem, pf_sem, near_sem, x_sem, vs_sem, vr_sem):
    f, me = lax.axis_index("frag"), lax.axis_index("dev")
    chip, core = me // 2, lax.rem(me, 2)
    far0 = (1 - chip) * 2 + core
    far1 = (1 - chip) * 2 + 1 - core
    near = chip * 2 + 1 - core
    peers = (far0, far1, near)

    def a_copy(p, slot):
        return pltpu.make_async_copy(a_hbm.at[p], a_buf.at[slot], a_sem.at[slot])

    small = [pltpu.make_async_copy(x, y, in_sem.at[k]) for k, (x, y) in enumerate(
        [(co_hbm, co_ref), (cv_hbm, cv_ref), (eo_hbm, eo_ref), (ev_hbm, ev_ref)])]
    for cp in small[:2]:
        cp.start()
    a_copy(0, 0).start()
    a_copy(1, 1).start()
    if PH > A1:
        p_far[:, :, :, PH - 16:, :] = jnp.zeros((2, NP, 3, 16, L), BF16)
    barrier = pltpu.get_barrier_semaphore()
    for d in peers:
        pl.semaphore_signal(barrier, inc=1, device_id=(f, d), device_id_type=MESH)
    for cp in small[:2]:
        cp.wait()
    for s in range(2, SLOTS):
        a_copy(s, s).start()
    for cp in small[2:]:
        cp.start()

    co, cv = co_ref[...], cv_ref[...]
    mod = lambda x, d: x - d * _div(x, d)
    co_pad = jnp.pad(co.astype(F32), ((0, O), (0, 256 - N)))
    l1[...] = (co_pad + pltpu.roll(pltpu.roll(co_pad, O, axis=0), N, axis=1)).astype(BF16)[:, :2 * N]
    cv_t = jnp.pad(cv.astype(F32), ((0, L - V), (0, L - N))).T
    cv_pad = jnp.pad(cv_t, ((0, 0), (0, JB - L)))
    for jj in range(OD):
        w2[jj * L:(jj + 1) * L, :] = (pltpu.roll(cv_pad, V * jj, axis=1) if jj else cv_pad).astype(BF16)
    lp[...] = cv[:PH]

    def build_l3():
        twice = _dot(_onehot(_div(_rows((GR, V)), PC) == _cols((GR, V))), cv)
        twice = jnp.pad(twice, ((0, 0), (0, 256 - N)))
        l3[...] = jnp.where(mod(_rows((GR, 256)), PC) == 0, twice, pltpu.roll(twice, N, axis=1)).astype(BF16)[:, :PC * N]

    def spread_co(slot0, slot1):
        return _spread(
            co, lambda x: _div(x, 16) * 2 + mod(x, 2),
            lambda y: jnp.where(y < NC * 16, slot0, slot1).astype(F32) * NP + _div(mod(y, NC * 16), 16) * PC + mod(y, PC),
            lambda x, y: _div(mod(x, 16), 2) == _div(mod(y, 16), PC), (8 * O, 2 * NC * 16))

    def p_copy(p, k):
        return pltpu.make_async_remote_copy(
            src_ref=p_send.at[p, k, :, pl.ds(0, A1)], dst_ref=p_far.at[k, p, :, pl.ds(0, A1)], send_sem=ps_sem.at[p, k],
            recv_sem=pf_sem.at[k, p], device_id=(f, peers[k]), device_id_type=MESH)

    def x_copy(c):
        return pltpu.make_async_remote_copy(
            src_ref=g_send.at[c, 1, pl.ds(U0 * 16, XR)], dst_ref=x_near.at[c], send_sem=send_sem.at[c, 0],
            recv_sem=x_sem.at[c], device_id=(f, near), device_id_type=MESH)

    def n_copy(c):
        return pltpu.make_async_remote_copy(
            src_ref=g_send.at[c, 2], dst_ref=g_near.at[c], send_sem=send_sem.at[c, 1],
            recv_sem=near_sem.at[c], device_id=(f, near), device_id_type=MESH)

    def v_copy(g):
        return pltpu.make_async_remote_copy(
            src_ref=v_send.at[g, :, pl.ds(0, VT)], dst_ref=v_recv.at[g, :, pl.ds(0, VT)], send_sem=vs_sem.at[g],
            recv_sem=vr_sem.at[g], device_id=(f, far0), device_id_type=MESH)

    def first_step(slot, buf, q):
        x0 = jnp.pad(a_buf[slot, q:q + 2].reshape(2 * N, N), ((0, 0), (0, L - N)))
        x1 = jnp.pad(a_buf[slot, q + 2:q + 4].reshape(2 * N, N), ((0, 0), (0, L - N)))
        t = _dot(l1[...], jnp.concatenate([x0, x1], axis=1))
        buf[q * O:(q + 2) * O, :] = t[:, :L]
        buf[(q + 2) * O:(q + 4) * O, :] = t[:, L:]

    def second_step(buf, row):
        x = [jnp.concatenate([buf[pl.ds(d * OD + jj, N, stride=O), :].astype(BF16) for d in range(NDEV)], axis=0)
             for jj in range(OD)]
        h0 = _dot(jnp.concatenate(x[:4], axis=1), w2[:4 * L, :256]).astype(BF16)
        h1 = _dot(jnp.concatenate(x[2:], axis=1), w2[2 * L:, 256:]).astype(BF16)
        for d in range(NDEV):
            h_s[d, row * N:(row + 1) * N, :256] = h0[d * N:(d + 1) * N]
            h_s[d, row * N:(row + 1) * N, 256:] = h1[d * N:(d + 1) * N]

    def piece(p, row):
        for k in range(2):
            g = _dot(lp[...], h_s[peers[k], row * N:(row + 1) * N, :]).astype(BF16)
            for n in range(3):
                p_send[p, k, n] = g[:, n * L:(n + 1) * L]

    def third_step(c, k):
        r0 = U0 * 16 if k < 2 else 0
        g = _dot(l3[r0:, :], h_s[(far0, far1, near, me)[k]]).astype(BF16)
        if k < 3:
            g_send[c, k, r0:, :] = g
        else:
            g_own[c] = g

    def prefetch(p, slot):
        @pl.when(p + SLOTS < NP)
        def _():
            a_copy(p + SLOTS, slot).start()
            a_copy(p + 1 + SLOTS, slot + 1).start()

    def send_piece(p):
        p_copy(p, 0).start()
        p_copy(p, 1).start()

    a_copy(0, 0).wait()
    for q in range(0, N, 4):
        first_step(0, t0_s, q)
    second_step(t0_s, 0)
    piece(0, 0)
    pl.semaphore_wait(barrier, 3)
    send_piece(0)
    a_copy(1, 1).wait()
    for q in range(0, N, 4):
        first_step(1, t1_s, q)
    build_l3()
    prefetch(0, 0)

    def chunk(c, _):
        p = c * PC
        slot = lax.rem(p, SLOTS)
        a_copy(p, slot).wait()
        for n, q in enumerate(range(0, N, 4)):
            if n == 1:
                second_step(t1_s, 1)
            first_step(slot, t0_s, q)
            if n == 8:
                piece(p - 1, 1)
            if n in (11, 14, 17, 20):
                third_step(c - 1, (n - 11) // 3)
        x_copy(c - 1).start()
        send_piece(p - 1)
        a_copy(p + 1, slot + 1).wait()
        for n, q in enumerate(range(0, N, 4)):
            if n == 1:
                second_step(t0_s, 0)
            first_step(slot + 1, t1_s, q)
            if n == 12:
                piece(p, 0)
        send_piece(p)
        prefetch(p, slot)
        return 0

    lax.fori_loop(1, NC, chunk, 0)
    last = NC - 1
    second_step(t1_s, 1)
    third_step(last, 1)
    x_copy(last).start()
    third_step(last, 0)
    piece(NP - 1, 1)
    send_piece(NP - 1)
    third_step(last, 2)
    third_step(last, 3)

    l4[...] = spread_co(me, near)

    def octet(own, other, t, t_other):
        rows = pl.ds(pl.multiple_of(t * 16, 16), 16)
        orows = pl.ds(pl.multiple_of(t_other * 16, 16), 16)
        return jnp.concatenate([own[:, rows].reshape(NC * 16, JB), other[:, orows].reshape(NC * 16, JB)], axis=0)

    for c in range(NC):
        x_copy(c).wait_recv()

    def partial(t, g0, g1):
        v = _dot(l4[g0 * 16:g1 * 16, :], octet(g_send.at[:, 0], x_near, t, t - U0))
        r0 = VO if t == U0 else 0
        r1 = min(16, V * 2 - t * 16)
        at = t * 16 - A1 * 2
        for g in range(g0, g1):
            row = (g - g0) * 16
            for n in range(3):
                v_send[g, n, at + r0:at + r1, :] = v[row + r0:row + r1, n * L:(n + 1) * L]

    for g0, g1 in ((0, 3), (3, IG)):
        for t in range(U0, AO):
            partial(t, g0, g1)
        for g in range(g0, g1):
            v_copy(g).start()
    for c in range(NC):
        n_copy(c).start()

    l4f[...] = _spread(
        co, lambda x: _div(x, 32) * 2 + mod(x, 2),
        lambda y: jnp.where(y < FK, far0, far1).astype(F32) * NP + _div(mod(y, FK), 16),
        lambda x, y: _div(mod(x, 32), 2) == mod(y, 16), (16 * O, 2 * FK))

    for cp in small[2:]:
        cp.wait()
    ev = jnp.broadcast_to(ev_ref[...], (L, V))
    ev = jnp.pad(ev, ((0, 0), (0, L - V)))
    pair = ev + ev.T
    inside = (_rows((80, L)) < V) & (_cols((80, L)) < V)

    def recip(i, _):
        for jj in range(OD):
            den = (eo_ref[i] + eo_ref[me * OD + jj]) - pair[:80]
            r_s[i * OD + jj] = jnp.where(inside, 1.0 / den, 0.0)
        return 0

    lax.fori_loop(0, O, recip, 0)

    for c in range(NC):
        n_copy(c).wait_recv()

    def contract(t, _):
        v = _dot(l4[...], octet(g_own, g_near, t, t))
        rows = pl.ds(pl.multiple_of(t * 16, 16), 16)
        for g in range(IG):
            for n in range(3):
                v_s[g, n, rows, :] = v[g * 16:(g + 1) * 16, n * L:(n + 1) * L]
        return 0

    lax.fori_loop(0, AO, contract, 0)
    for p in range(NP):
        for k in range(2):
            p_copy(p, k).wait_recv()

    for u in range(U2):
        for n in range(3):
            v = _dot(l4f[...], p_far[:, :, n, u * 16:(u + 1) * 16, :].reshape(2 * FK, L))
            for g in range(IG):
                v_s[g, n, u * 32:(u + 1) * 32, :] += v[g * 32:(g + 1) * 32]

    for p in range(NP):
        p_copy(p, 0).wait_send()
        p_copy(p, 1).wait_send()
    for c in range(NC):
        x_copy(c).wait_send()
        n_copy(c).wait_send()
    def energy(g, _):
        v_copy(g).wait()
        v_s[g, :, A1 * 2:V * 2, :] += v_recv[g, :, :VT]
        lane = lax.broadcasted_iota(jnp.int32, (80, L), 1)
        for ii in range(2):
            i = g * 2 + ii
            tiles = [v_s[g, n, pl.ds(ii, 80, stride=2), :] for n in range(3)]
            for jj in range(OD):
                t, off = divmod(V * jj, L)
                m = pltpu.roll(tiles[t], (L - off) % L, axis=1) if off else tiles[t]
                if off + V > L:
                    m = jnp.where(lane < L - off, m, pltpu.roll(tiles[t + 1], L - off, axis=1))
                mt = jnp.pad(m, ((0, L - 80), (0, 0))).T[:80]
                term = m * (2.0 * m - mt) * r_s[i * OD + jj]
                e_s[jj, pl.ds(pl.multiple_of(i * 8, 8), 8), :] = jnp.sum(term.reshape(10, 8, L), axis=0)
        return 0

    lax.fori_loop(0, IG, energy, 0)
    for jj in range(OD):
        tot = e_s[jj, pl.ds(0, O, stride=8), :]
        for s in range(1, 8):
            tot = tot + e_s[jj, pl.ds(s, O, stride=8), :]
        col = jnp.sum(jnp.pad(tot, ((0, 32 - O), (0, 0))).T, axis=0, keepdims=True)
        out_ref[jj:jj + 1, :] = col[:, :O]


def solution(mesh):
    def per_device(a_ints, c_occ, c_vir, eps_occ, eps_vir):
        vm = pl.BlockSpec(memory_space=pltpu.VMEM)
        e = pl.pallas_call(
            kernel,
            out_shape=pltpu.VMEM((OD, O), F32),
            in_specs=[pl.BlockSpec(memory_space=pltpu.HBM)] * 5,
            out_specs=vm,
            scratch_shapes=[
                pltpu.VMEM((O, N), BF16),
                pltpu.VMEM((V, N), BF16),
                pltpu.SMEM((O,), F32),
                pltpu.VMEM((1, V), F32),
                pltpu.VMEM((SLOTS, N, N, N), BF16),
                pltpu.VMEM((2 * O, 2 * N), BF16),
                pltpu.VMEM((OD * L, JB), BF16),
                pltpu.VMEM((GR, PC * N), BF16),
                pltpu.VMEM((PH, N), BF16),
                pltpu.VMEM((8 * O, 2 * NC * 16), BF16),
                pltpu.VMEM((16 * O, 2 * FK), BF16),
                pltpu.VMEM((N * O, L), F32),
                pltpu.VMEM((N * O, L), F32),
                pltpu.VMEM((NDEV, PC * N, JB), BF16),
                pltpu.VMEM((NC, 3, GR, JB), BF16),
                pltpu.VMEM((NC, GR, JB), BF16),
                pltpu.VMEM((NC, GR, JB), BF16),
                pltpu.VMEM((NP, 2, 3, PH, L), BF16),
                pltpu.VMEM((2, NP, 3, PH, L), BF16),
                pltpu.VMEM((NC, XR, JB), BF16),
                pltpu.VMEM((IG, 3, VR, L), F32),
                pltpu.VMEM((IG, 3, VR, L), F32),
                pltpu.VMEM((IG, 3, AO * 16, L), F32),
                pltpu.VMEM((O * OD, 80, L), F32),
                pltpu.VMEM((OD, O * 8, L), F32),
                pltpu.SemaphoreType.DMA((SLOTS,)),
                pltpu.SemaphoreType.DMA((4,)),
                pltpu.SemaphoreType.DMA((NC, 2)),
                pltpu.SemaphoreType.DMA((NP, 2)),
                pltpu.SemaphoreType.DMA((2, NP)),
                pltpu.SemaphoreType.DMA((NC,)),
                pltpu.SemaphoreType.DMA((NC,)),
                pltpu.SemaphoreType.DMA((IG,)),
                pltpu.SemaphoreType.DMA((IG,)),
            ],
            compiler_params=pltpu.CompilerParams(
                collective_id=0, has_side_effects=True, vmem_limit_bytes=60 * 2**20),
        )(a_ints, c_occ.T, c_vir.T, eps_occ, eps_vir.reshape(1, V))
        return e.T

    return jax.shard_map(
        per_device,
        mesh=mesh,
        in_specs=(P(("frag", "dev")), P("frag"), P("frag"), P("frag"), P("frag")),
        out_specs=P("frag", "dev"),
        check_vma=False,
    )
```
